32 devices in a mesh: section: 16 (over z, y, core), dp: 2 (over x).
Axes of the slice: x: 2, y: 2, z: 4, core: 2. Of those that a mesh axis runs over, the one named last changes fastest.
Arguments:
- layer_in: bfloat16 [16, 256, 5120], P('section', 'dp'), may hold values from -6 to 6
- latent: bfloat16 [16, 256, 384], P('section', 'dp'), may hold values from -6 to 6
- mix_grad: bfloat16 [16, 256, 5120], P('section', 'dp'), may hold values from -0.375 to 0.375
- down_proj: bfloat16 [16, 5120, 384], P('section', 'dp'), may hold values from -0.078125 to 0.078125
- up_proj: bfloat16 [16, 384, 5120], P('section', None, 'dp'), may hold values from -0.3125 to 0.3125
- norm_gain: bfloat16 [16, 5120], P('section', 'dp'), may hold values from 0.5 to 1.5
- mix_weight: float32 [16, 8], P('section'), may hold values from 0.2 to 1
Outputs:
- up_grad: bfloat16 [16, 384, 5120], P('section', None, 'dp')
- down_grad: bfloat16 [16, 5120, 384], P('section', 'dp')
- gain_grad: float32 [16, 5120], P('section', 'dp')
- mixing_grad: float32 [16, 8], P('section')
The draws below stay inside these ranges and needn't reach their ends.
All inputs are finite; a program needn't handle non-finite values.
Results may differ from the reference program's by a relative error of at most 0.0064.
Values may be sent and summed in bfloat16 or wider, within the bound.
A program may use at most 128 MiB of HBM per device.

```python
import jax
import jax.numpy as jnp
from jax import lax

D = 5120
R = 384
MIXES = 8
LAYERS = 16
TOKENS = 256


def steps_of(stream_key, dims, cuts, least, largest):
    def one(axis_at, blocks):
        steps = jax.random.uniform(jax.random.fold_in(jax.random.fold_in(stream_key, 6), axis_at), (blocks,), jnp.float32, least / len(cuts), largest / len(cuts))
        return jnp.repeat(jnp.exp(steps), dims[axis_at] // blocks).reshape((-1,) + (1,) * (len(dims) - axis_at - 1))

    level = one(*cuts[0])
    for cut in cuts[1:]:
        level = level * one(*cut)
    return level


def gaussian(stream_key, extent, scale, bound, split=(), held_as=jnp.bfloat16):
    loudness = steps_of(stream_key, extent, split, -0.22, 0.18) if split else 1.0
    array = jax.random.normal(stream_key, extent, jnp.float32) * scale * loudness
    return jnp.minimum(jnp.maximum(array, -bound), bound).astype(held_as)


def setup_inputs(seed: int = 0) -> dict:
    arg_keys = jax.random.split(jax.random.key(seed), 8)
    layer_in = gaussian(arg_keys[0], (LAYERS, TOKENS, D), 1.0, 6.0, ((0, 16), (1, 2)))
    latent = gaussian(arg_keys[1], (LAYERS, TOKENS, R), 1.0, 6.0, ((0, 16), (1, 2)))
    mix_grad = gaussian(arg_keys[2], (LAYERS, TOKENS, D), (TOKENS ** -0.5), 0.375, ((0, 16), (1, 2)))
    down_proj = gaussian(arg_keys[3], (LAYERS, D, R), D ** -0.5, 0.078125, ((0, 16), (1, 2)))
    up_proj = gaussian(arg_keys[4], (LAYERS, R, D), R ** -0.5, 0.3125, ((0, 16), (2, 2)))
    norm_gain = jnp.clip(1.0 + 0.1 * jax.random.normal(arg_keys[5], (LAYERS, D), jnp.float32), 0.5, 1.5).astype(jnp.bfloat16)
    mix_weight = jnp.clip(0.2 + 0.8 * jax.random.uniform(arg_keys[6], (LAYERS, MIXES), jnp.float32) ** steps_of(arg_keys[6], (LAYERS, MIXES), ((0, 16),), -0.2, 0.2), 0.2, 1.0)
    return {"layer_in": layer_in, "latent": latent, "mix_grad": mix_grad, "down_proj": down_proj, "up_proj": up_proj, "norm_gain": norm_gain, "mix_weight": mix_weight}


epsilon = 1e-06
root_coef = 0.7978845608028654

def gelu_pair(values):
    tangent = jnp.tanh(root_coef * (values + 0.044715 * values * values * values))
    result = 0.5 * values * (1.0 + tangent)
    slopes = 0.5 * (1.0 + tangent) + 0.5 * values * (1.0 - tangent * tangent) * root_coef * (1.0 + 3.0 * 0.044715 * values * values)
    return (result, slopes)

def reference(layer_in, latent, mix_grad, down_proj, up_proj, norm_gain, mix_weight):
    stride = LAYERS // MIXES

    def one_section(index):
        inputs = lax.dynamic_index_in_dim(layer_in, index, 0, False).astype(jnp.float32)
        mean_sq = lax.optimization_barrier(jnp.mean(inputs * inputs, axis=1, keepdims=True))
        inv_rms = lax.rsqrt(mean_sq + epsilon)
        scaled = inputs * inv_rms
        gain_row = lax.dynamic_index_in_dim(norm_gain, index, 0, False).astype(jnp.float32)
        normed = (scaled * gain_row).astype(jnp.bfloat16)
        latent_row = lax.dynamic_index_in_dim(latent, index, 0, False).astype(jnp.float32)
        activated, slopes = gelu_pair(latent_row)
        act_half = activated.astype(jnp.bfloat16)
        up_block = lax.dynamic_index_in_dim(up_proj, index, 0, False)
        down_block = lax.dynamic_index_in_dim(down_proj, index, 0, False)
        layer_out = inputs + jnp.dot(act_half, up_block, preferred_element_type=jnp.float32)
        weight_row = lax.dynamic_index_in_dim(mix_weight, index, 0, False)
        grad_sum = jnp.zeros(inputs.shape, jnp.float32)
        products = []
        for member in range(MIXES):
            target = index + member * stride
            inside = (target < LAYERS).astype(jnp.float32)
            clamped = jnp.minimum(target, LAYERS - 1).astype(jnp.int32)
            piece = lax.dynamic_index_in_dim(mix_grad, clamped, 0, False).astype(jnp.float32) * inside
            products.append(jnp.sum(piece * layer_out))
            grad_sum = grad_sum + weight_row[member] * piece
        grad_half = grad_sum.astype(jnp.bfloat16)
        act_grad = jnp.dot(grad_half, up_block.T, preferred_element_type=jnp.float32)
        latent_grad = (act_grad * slopes).astype(jnp.bfloat16)
        up_grad = jnp.dot(act_half.T, grad_half, preferred_element_type=jnp.float32).astype(jnp.bfloat16)
        down_grad = jnp.dot(normed.T, latent_grad, preferred_element_type=jnp.float32).astype(jnp.bfloat16)
        norm_grad = jnp.dot(latent_grad, down_block.T, preferred_element_type=jnp.float32)
        gain_grad = lax.optimization_barrier(jnp.sum(norm_grad * scaled, axis=0))
        return (up_grad, down_grad, gain_grad, jnp.stack(products))
    up_grad, down_grad, gain_grad, mixing_grad = lax.map(one_section, jnp.arange(LAYERS, dtype=jnp.int32))
    return (up_grad, down_grad, gain_grad, mixing_grad)
```

```python
import functools

import jax
import jax.numpy as jnp
from jax import lax
from jax.experimental import pallas as pl
from jax.experimental.pallas import tpu as pltpu
from jax.sharding import PartitionSpec as P

MIXES = 8
LEVELS = MIXES // 2
CHUNK = 32
TILE = 640

epsilon = 1e-06
root_coef = 0.7978845608028654
MESH = pl.DeviceIdType.MESH
F32 = jnp.float32
BF16 = jnp.bfloat16


def gelu_pair(values):
    tangent = jnp.tanh(root_coef * (values + 0.044715 * values * values * values))
    result = 0.5 * values * (1.0 + tangent)
    slopes = 0.5 * (1.0 + tangent) + 0.5 * values * (1.0 - tangent * tangent) * root_coef * (
        1.0 + 3.0 * 0.044715 * values * values
    )
    return (result, slopes)


def fold(values):
    rows, cols = values.shape
    total = jnp.sum(values.reshape(rows // 8, 8, cols), axis=0)
    out = total[:, 0:128]
    for at in range(128, cols, 128):
        out = out + total[:, at : at + 128]
    return out


def kernel(
    n, stride,
    x_ref, lat_ref, g_ref, down_ref, up_ref, gain_ref, wrel_ref,
    upg_ref, dng_ref, gaing_ref, mix_ref,
    xo, cin, latv, gb, inv, actv, slopes, lown, lpeer, sacc, sout, og, mixacc,
    mst, mrecv_y, msx, mrecv_dp, wpeer, upv, downv, apart, apown, rsb, lg,
    loc, gsend, grecv, xsend, xrecv, tsend, trecv, isend, irecv, wsem, zsend, zrecv,
    ssend, srecv, lsend, lrecv, rsend, rrecv, asend, arecv, mysem, msend, mrecv,
):
    own_rows, width = x_ref.shape
    feats = width // n
    half = own_rows // 2
    subs = half // CHUNK
    chunks = n * subs
    tiles = feats // TILE

    sec = lax.axis_index("section")
    x = lax.axis_index("dp")
    q = sec // stride
    res = sec % stride
    a = q // 2
    h = q % 2

    def at(level, side):
        return (2 * level + side) * stride + res

    me_y = sec
    other_y = at(a, 1 - h)
    above = at(a + 1, h)
    below = at(a - 1, h)

    def dev(section, dp):
        return {"section": section, "dp": dp}

    def to(k):
        return lax.rem(x + k, n)

    def source(k):
        return lax.rem(x + n - k, n)

    def remote(src, dst, ssem, rsem, section, dp):
        return pltpu.make_async_remote_copy(
            src_ref=src, dst_ref=dst, send_sem=ssem, recv_sem=rsem,
            device_id=dev(section, dp), device_id_type=MESH,
        )

    def rows(start, size, unit):
        return pl.ds(pl.multiple_of(start, unit), size)

    barrier = pltpu.get_barrier_semaphore()
    for k in range(n):
        for e in range(2):
            if k or e:
                pl.semaphore_signal(
                    barrier, inc=1, device_id=dev(other_y if e else me_y, to(k)), device_id_type=MESH
                )

    @pl.when(a > 0)
    def _():
        pl.semaphore_signal(barrier, inc=1, device_id=dev(below, x), device_id_type=MESH)

    @pl.when(a < LEVELS - 1)
    def _():
        pl.semaphore_signal(barrier, inc=1, device_id=dev(above, x), device_id_type=MESH)

    own_cols = rows(x * feats, feats, 128)
    own_block = rows(x * own_rows, own_rows, own_rows)
    local = [
        pltpu.make_async_copy(
            g_ref.at[rows(h * half, half, half), own_cols], gb.at[h, rows(x * half, half, half)], loc.at[0]
        ),
        pltpu.make_async_copy(lat_ref, latv.at[own_block], loc.at[1]),
        pltpu.make_async_copy(x_ref, xo, loc.at[2]),
        pltpu.make_async_copy(x_ref.at[:, own_cols], cin.at[own_block], loc.at[3]),
        pltpu.make_async_copy(up_ref, upv, loc.at[4]),
        pltpu.make_async_copy(down_ref, downv, loc.at[5]),
    ]
    for copy in local:
        copy.start()

    neighbours = jnp.where(a > 0, 1, 0) + jnp.where(a < LEVELS - 1, 1, 0)
    pl.semaphore_wait(barrier, 2 * n - 1 + neighbours)

    sends = []

    def go(copy):
        copy.start()
        sends.append(copy)
        return copy

    def g_copy(k, e):
        side = 1 - h if e else h
        return remote(
            g_ref.at[rows(side * half, half, half), rows(to(k) * feats, feats, 128)],
            gb.at[h, rows(x * half, half, half)],
            gsend.at[e * n + k], grecv.at[e * n + k],
            other_y if e else me_y, to(k),
        )

    def g_arrival(k, e):
        slot = 1 - h if e else h
        dst = gb.at[slot, rows(source(k) * half, half, half)]
        return remote(dst, dst, gsend.at[e * n + k], grecv.at[e * n + k], me_y, to(k) if k else x)

    go(g_copy(0, 1))
    w_copy = go(remote(wrel_ref, wpeer, wsem.at[0], wsem.at[1], other_y, x))
    for k in range(1, n):
        go(remote(lat_ref, latv.at[own_block], tsend.at[k], trecv.at[k], me_y, to(k)))
        go(g_copy(k, 0))
        go(g_copy(k, 1))
    for k in range(1, n):
        go(remote(
            x_ref.at[:, rows(to(k) * feats, feats, 128)], cin.at[own_block],
            xsend.at[k], xrecv.at[k], me_y, to(k),
        ))

    def arrival(dst, ssem, rsem):
        return remote(dst, dst, ssem, rsem, other_y, x)

    def chunk_at(c):
        k, sub = divmod(c, subs)
        return source(k), k, sub

    def z_copy(slot, c):
        j, _, sub = chunk_at(c)
        span = rows(j * half + sub * CHUNK, CHUNK, CHUNK)
        return remote(
            gb.at[slot, span], gb.at[slot + 2, span], zsend.at[slot, c], zrecv.at[slot + 2, c], below, x
        )

    def z_arrival(slot, c):
        j, _, sub = chunk_at(c)
        dst = gb.at[slot, rows(j * half + sub * CHUNK, CHUNK, CHUNK)]
        return remote(dst, dst, zsend.at[slot - 2, c], zrecv.at[slot, c], other_y, x)

    def flow(c):
        j, k, sub = chunk_at(c)
        if sub == 0:
            if k == 0:
                local[0].wait()
            else:
                g_arrival(k, 0).wait_recv()
            g_arrival(k, 1).wait_recv()

        @pl.when(a > 0)
        def _():
            z_copy(0, c).start()
            z_copy(1, c).start()

        for d in range(1, LEVELS):
            @pl.when(a + d < LEVELS)
            def _():
                for slot in (2 * d, 2 * d + 1):
                    z_arrival(slot, c).wait_recv()
                    if d < LEVELS - 1:
                        @pl.when(a > 0)
                        def _():
                            z_copy(slot, c).start()

    def weight(ref, slot):
        return ref[slot : slot + 1, 0:1]

    def combine(c):
        j, _, sub = chunk_at(c)
        span = rows(j * half + sub * CHUNK, CHUNK, CHUNK)
        for d in range(LEVELS):
            @pl.when(a + d < LEVELS)
            def _():
                @pl.loop(0, tiles)
                def _(t):
                    cols = rows(t * TILE, TILE, 128)
                    first = gb[2 * d, span, cols].astype(F32)
                    second = gb[2 * d + 1, span, cols].astype(F32)
                    for bb, ref in ((0, wrel_ref), (1, wpeer)):
                        value = weight(ref, 2 * d) * first + weight(ref, 2 * d + 1) * second
                        if d:
                            value = sacc[bb, :, cols] + value
                        sacc[bb, :, cols] = value

        @pl.loop(0, tiles)
        def _(t):
            cols = rows(t * TILE, TILE, 128)
            og[rows(j * own_rows + h * half + sub * CHUNK, CHUNK, CHUNK), cols] = sacc[0, :, cols].astype(BF16)
            sout[span, cols] = sacc[1, :, cols].astype(BF16)

        go(remote(
            sout.at[span], og.at[rows(j * own_rows + h * half + sub * CHUNK, CHUNK, CHUNK)],
            ssend.at[c], srecv.at[c], other_y, x,
        ))

    def s_arrival(c):
        j, _, sub = chunk_at(c)
        return arrival(
            og.at[rows(j * own_rows + (1 - h) * half + sub * CHUNK, CHUNK, CHUNK)], ssend.at[c], srecv.at[c]
        )

    def inner(c):
        j, k, sub = chunk_at(c)
        span = rows(j * half + sub * CHUNK, CHUNK, CHUNK)
        own_span = rows(j * own_rows + h * half + sub * CHUNK, CHUNK, CHUNK)
        if sub == 0:
            arrival(lpeer.at[rows(j * half, half, half)], lsend.at[k], lrecv.at[k]).wait_recv()
        for d in range(LEVELS):
            @pl.when(a + d < LEVELS)
            def _():
                @pl.loop(0, tiles)
                def _(t):
                    cols = rows(t * TILE, TILE, 128)
                    mine = lown[own_span, cols].astype(F32)
                    theirs = lpeer[span, cols].astype(F32)
                    for slot in (2 * d, 2 * d + 1):
                        values = gb[slot, span, cols].astype(F32)
                        mixacc[slot] += fold(values * mine)
                        mixacc[8 + slot] += fold(values * theirs)

    mixacc[...] = jnp.zeros_like(mixacc)
    local[2].wait()

    def square(t, total):
        part = xo[:, rows(t * TILE, TILE, 128)].astype(F32)
        part = part * part
        for at_col in range(0, TILE, 128):
            total = total + part[:, at_col : at_col + 128]
        return total

    lanes = lax.fori_loop(0, width // TILE, square, jnp.zeros((own_rows, 128), F32))
    mean_sq = jnp.sum(lanes, axis=1, keepdims=True) / width
    inv[own_block] = jnp.broadcast_to(lax.rsqrt(mean_sq + epsilon), (own_rows, 128))
    for k in range(1, n):
        go(remote(inv.at[own_block], inv.at[own_block], isend.at[k], irecv.at[k], me_y, to(k)))

    arrival(wpeer, wsem.at[0], wsem.at[1]).wait_recv()
    flow(0)

    local[1].wait()
    for k in range(1, n):
        arrival(latv.at[rows(source(k) * own_rows, own_rows, own_rows)], tsend.at[k], trecv.at[k]).wait_recv()
    _, own_slopes = gelu_pair(latv[own_block].astype(F32))
    slopes[...] = own_slopes
    for j in range(n):
        block = slice(j * own_rows, (j + 1) * own_rows)
        values, _ = gelu_pair(latv[block].astype(F32))
        actv[block] = values.astype(BF16)
    local[4].wait()
    local[3].wait()

    def layer_out(k):
        j = source(k)
        block = rows(j * own_rows, own_rows, own_rows)
        if k:
            arrival(cin.at[block], xsend.at[k], xrecv.at[k]).wait_recv()

        @pl.loop(0, tiles)
        def _(t):
            cols = rows(t * TILE, TILE, 128)
            branch = jnp.dot(actv[block, :], upv[:, cols], preferred_element_type=F32)
            lown[block, cols] = (cin[block, cols].astype(F32) + branch).astype(BF16)

        go(remote(
            lown.at[rows(j * own_rows + (1 - h) * half, half, half)], lpeer.at[rows(j * half, half, half)],
            lsend.at[k], lrecv.at[k], other_y, x,
        ))

    def act_block(k):
        j = source(k)
        for sub in range(subs):
            s_arrival(k * subs + sub).wait_recv()
        part = lax.dot_general(
            og[rows(j * own_rows, own_rows, own_rows), :], upv[...], (((1,), (1,)), ((), ())),
            preferred_element_type=F32,
        )
        if k == 0:
            apown[...] = part
        else:
            apart[k] = part.astype(BF16)
            go(remote(apart.at[k], rsb.at[k], rsend.at[k], rrecv.at[k], me_y, j))

    layer_out(0)
    combine(0)
    for c in range(1, chunks):
        k, sub = divmod(c, subs)
        flow(c)
        combine(c)
        inner(c - 1)
        if sub == 0:
            layer_out(k)
            act_block(k - 1)
    act_block(n - 1)
    inner(chunks - 1)

    for bb in range(2):
        for slot in range(8):
            mst[bb, slot : slot + 1] = jnp.sum(mixacc[8 * bb + slot], axis=0, keepdims=True)
    go(remote(mst.at[1], mrecv_y, mysem.at[0], mysem.at[1], other_y, x))

    total = apown[...]
    for k in range(1, n):
        arrival(rsb.at[k], rsend.at[k], rrecv.at[k]).wait_recv()
        total = total + rsb[k].astype(F32)
    lg[own_block] = (total * slopes[...]).astype(BF16)
    for k in range(1, n):
        go(remote(lg.at[own_block], lg.at[own_block], asend.at[k], arecv.at[k], me_y, to(k)))

    arrival(mrecv_y, mysem.at[0], mysem.at[1]).wait_recv()
    msx[...] = mst[0] + mrecv_y[...]
    for k in range(1, n):
        go(remote(msx, mrecv_dp.at[k], msend.at[k], mrecv.at[k], me_y, to(k)))

    @pl.loop(0, tiles)
    def _(t):
        cols = rows(t * TILE, TILE, 128)
        upg_ref[:, cols] = lax.dot_general(
            actv[...], og[:, cols], (((0,), (0,)), ((), ())), preferred_element_type=F32
        ).astype(BF16)

    mixed = msx[...]
    for k in range(1, n):
        arrival(mrecv_dp.at[k], msend.at[k], mrecv.at[k]).wait_recv()
        mixed = mixed + mrecv_dp[k]
    mix_ref[...] = mixed

    for k in range(1, n):
        block = rows(source(k) * own_rows, own_rows, own_rows)
        arrival(inv.at[block], isend.at[k], irecv.at[k]).wait_recv()
        arrival(lg.at[block], asend.at[k], arecv.at[k]).wait_recv()
    local[5].wait()

    @pl.loop(0, tiles)
    def _(t):
        cols = rows(t * TILE, TILE, 128)
        scaled = cin[:, cols].astype(F32) * inv[:, 0:1]
        normed = (scaled * gain_ref[:, cols].astype(F32)).astype(BF16)
        dng_ref[rows(t * TILE, TILE, 128), :] = lax.dot_general(
            normed, lg[...], (((0,), (0,)), ((), ())), preferred_element_type=F32
        ).astype(BF16)
        norm_grad = lax.dot_general(
            lg[...], downv[rows(t * TILE, TILE, 128), :], (((1,), (1,)), ((), ())),
            preferred_element_type=F32,
        )
        gaing_ref[:, cols] = jnp.sum(norm_grad * scaled, axis=0, keepdims=True)

    for copy in sends:
        copy.wait_send()

    @pl.when(a > 0)
    def _():
        for c in range(chunks):
            z_copy(0, c).wait_send()
            z_copy(1, c).wait_send()
        for d in range(1, LEVELS - 1):
            @pl.when(a + d < LEVELS)
            def _():
                for c in range(chunks):
                    z_copy(2 * d, c).wait_send()
                    z_copy(2 * d + 1, c).wait_send()


def local(layer_in, latent, mix_grad, down_proj, up_proj, norm_gain, mix_weight):
    _, own_rows, width = layer_in.shape
    n = lax.axis_size("dp")
    stride = lax.axis_size("section") // MIXES
    latents = latent.shape[2]
    feats = width // n
    tokens = own_rows * n
    chunks = tokens // 2 // CHUNK
    side = (lax.axis_index("section") // stride) % 2
    row = mix_weight[0]
    zero = jnp.zeros((1,), F32)
    rel = jnp.where(side == 1, jnp.concatenate([zero, row[:-1]]), row)
    rel = jnp.broadcast_to(rel[:, None], (MIXES, 128))
    dma = pltpu.SemaphoreType.DMA
    anyspace = pl.BlockSpec(memory_space=pl.ANY)
    vmem = pl.BlockSpec(memory_space=pltpu.VMEM)
    up_grad, down_grad, gain_grad, mixed = pl.pallas_call(
        functools.partial(kernel, n, stride),
        out_shape=(
            jax.ShapeDtypeStruct((latents, feats), BF16),
            jax.ShapeDtypeStruct((feats, latents), BF16),
            jax.ShapeDtypeStruct((1, feats), F32),
            jax.ShapeDtypeStruct((MIXES, 128), F32),
        ),
        in_specs=[anyspace] * 5 + [vmem] * 2,
        out_specs=(vmem,) * 4,
        scratch_shapes=[
            pltpu.VMEM((own_rows, width), BF16),
            pltpu.VMEM((tokens, feats), BF16),
            pltpu.VMEM((tokens, latents), BF16),
            pltpu.VMEM((MIXES, tokens // 2, feats), BF16),
            pltpu.VMEM((tokens, 128), F32),
            pltpu.VMEM((tokens, latents), BF16),
            pltpu.VMEM((own_rows, latents), F32),
            pltpu.VMEM((tokens, feats), BF16),
            pltpu.VMEM((tokens // 2, feats), BF16),
            pltpu.VMEM((2, CHUNK, feats), F32),
            pltpu.VMEM((tokens // 2, feats), BF16),
            pltpu.VMEM((tokens, feats), BF16),
            pltpu.VMEM((16, 8, 128), F32),
            pltpu.VMEM((2, 8, 128), F32),
            pltpu.VMEM((8, 128), F32),
            pltpu.VMEM((8, 128), F32),
            pltpu.VMEM((n, 8, 128), F32),
            pltpu.VMEM((8, 128), F32),
            pltpu.VMEM((latents, feats), BF16),
            pltpu.VMEM((feats, latents), BF16),
            pltpu.VMEM((n, own_rows, latents), BF16),
            pltpu.VMEM((own_rows, latents), F32),
            pltpu.VMEM((n, own_rows, latents), BF16),
            pltpu.VMEM((tokens, latents), BF16),
            dma((6,)),
            dma((2 * n,)), dma((2 * n,)),
            dma((n,)), dma((n,)),
            dma((n,)), dma((n,)),
            dma((n,)), dma((n,)),
            dma((2,)),
            dma((MIXES, chunks)), dma((MIXES, chunks)),
            dma((chunks,)), dma((chunks,)),
            dma((n,)), dma((n,)),
            dma((n,)), dma((n,)),
            dma((n,)), dma((n,)),
            dma((2,)),
            dma((n,)), dma((n,)),
        ],
        compiler_params=pltpu.CompilerParams(
            collective_id=0, has_side_effects=True, vmem_limit_bytes=60 * 1024 * 1024
        ),
    )(layer_in[0], latent[0], mix_grad[0], down_proj[0], up_proj[0], norm_gain, rel)
    sums = jnp.sum(mixed, axis=1)
    mixing = jnp.where(side == 1, jnp.concatenate([sums[1:], zero]), sums)
    return (up_grad[None], down_grad[None], gain_grad, mixing[None])


def solution(mesh):
    return jax.shard_map(
        local,
        mesh=mesh,
        in_specs=(
            P("section", "dp", None),
            P("section", "dp", None),
            P("section", "dp", None),
            P("section", "dp", None),
            P("section", None, "dp"),
            P("section", "dp"),
            P("section", None),
        ),
        out_specs=(
            P("section", None, "dp"),
            P("section", "dp", None),
            P("section", "dp"),
            P("section", None),
        ),
        check_vma=False,
    )
```

```python
import functools

import jax
import jax.numpy as jnp
from jax import lax
from jax.experimental import pallas as pl
from jax.experimental.pallas import tpu as pltpu
from jax.sharding import PartitionSpec as P

MIXES = 8
LEVELS = MIXES // 2
REACH = LEVELS - 1
SLOTS = 2 * REACH
CHUNK = 16
TILE = 640

epsilon = 1e-06
root_coef = 0.7978845608028654
MESH = pl.DeviceIdType.MESH
F32 = jnp.float32
BF16 = jnp.bfloat16


def gelu_pair(values):
    tangent = jnp.tanh(root_coef * (values + 0.044715 * values * values * values))
    result = 0.5 * values * (1.0 + tangent)
    slopes = 0.5 * (1.0 + tangent) + 0.5 * values * (1.0 - tangent * tangent) * root_coef * (
        1.0 + 3.0 * 0.044715 * values * values
    )
    return (result, slopes)


def fold(values):
    rows, cols = values.shape
    total = jnp.sum(values.reshape(rows // 8, 8, cols), axis=0)
    out = total[:, 0:128]
    for at in range(128, cols, 128):
        out = out + total[:, at : at + 128]
    return out


def kernel(
    n, stride,
    x_ref, lat_ref, g_ref, down_ref, up_ref, gain_ref, wrel_ref,
    upg_ref, dng_ref, gaing_ref, mix_ref,
    xo, cin, latv, gb, inv, actv, slopes, lown, lpeer, sacc, sout, og, mixacc,
    mst, mrecv_y, msx, mrecv_dp, wpeer, upv, downv, apart, apown, rsb, lg,
    wlow, llow, lowacc, s0out, s0in, mixlow, mlow, mlowin,
    loc, gsend, grecv, xsend, xrecv, tsend, trecv, isend, irecv, wsem, zsend, zrecv,
    wlsend, wlrecv, llsend, llrecv, s0send, s0recv, mlsend, mlrecv,
    ssend, srecv, lsend, lrecv, rsend, rrecv, asend, arecv, mysem, msend, mrecv,
):
    own_rows, width = x_ref.shape
    feats = width // n
    half = own_rows // 2
    subs = half // CHUNK
    chunks = n * subs
    tiles = feats // TILE

    sec = lax.axis_index("section")
    x = lax.axis_index("dp")
    q = sec // stride
    res = sec % stride
    a = q // 2
    h = q % 2

    def at(level, side):
        return (2 * level + side) * stride + res

    me_y = sec
    other_y = at(a, 1 - h)
    above = at(a + 1, h)
    below = at(a - 1, h)

    def dev(section, dp):
        return {"section": section, "dp": dp}

    def to(k):
        return lax.rem(x + k, n)

    def source(k):
        return lax.rem(x + n - k, n)

    def remote(src, dst, ssem, rsem, section, dp):
        return pltpu.make_async_remote_copy(
            src_ref=src, dst_ref=dst, send_sem=ssem, recv_sem=rsem,
            device_id=dev(section, dp), device_id_type=MESH,
        )

    def rows(start, size, unit):
        return pl.ds(pl.multiple_of(start, unit), size)

    barrier = pltpu.get_barrier_semaphore()
    for k in range(n):
        for e in range(2):
            if k or e:
                pl.semaphore_signal(
                    barrier, inc=1, device_id=dev(other_y if e else me_y, to(k)), device_id_type=MESH
                )

    @pl.when(a > 0)
    def _():
        pl.semaphore_signal(barrier, inc=1, device_id=dev(below, x), device_id_type=MESH)

    @pl.when(a < LEVELS - 1)
    def _():
        pl.semaphore_signal(barrier, inc=1, device_id=dev(above, x), device_id_type=MESH)

    own_cols = rows(x * feats, feats, 128)
    own_block = rows(x * own_rows, own_rows, own_rows)
    local = [
        pltpu.make_async_copy(
            g_ref.at[rows(h * half, half, half), own_cols], gb.at[h, rows(x * half, half, half)], loc.at[0]
        ),
        pltpu.make_async_copy(lat_ref, latv.at[own_block], loc.at[1]),
        pltpu.make_async_copy(x_ref, xo, loc.at[2]),
        pltpu.make_async_copy(x_ref.at[:, own_cols], cin.at[own_block], loc.at[3]),
        pltpu.make_async_copy(up_ref, upv, loc.at[4]),
        pltpu.make_async_copy(down_ref, downv, loc.at[5]),
    ]
    for copy in local:
        copy.start()

    neighbours = jnp.where(a > 0, 1, 0) + jnp.where(a < LEVELS - 1, 1, 0)
    pl.semaphore_wait(barrier, 2 * n - 1 + neighbours)

    sends = []

    def go(copy):
        copy.start()
        sends.append(copy)
        return copy

    def g_copy(k, e):
        side = 1 - h if e else h
        return remote(
            g_ref.at[rows(side * half, half, half), rows(to(k) * feats, feats, 128)],
            gb.at[h, rows(x * half, half, half)],
            gsend.at[e * n + k], grecv.at[e * n + k],
            other_y if e else me_y, to(k),
        )

    def g_arrival(k, e):
        slot = 1 - h if e else h
        dst = gb.at[slot, rows(source(k) * half, half, half)]
        return remote(dst, dst, gsend.at[e * n + k], grecv.at[e * n + k], me_y, to(k) if k else x)

    go(g_copy(0, 1))
    w_copy = go(remote(wrel_ref, wpeer, wsem.at[0], wsem.at[1], other_y, x))
    for k in range(1, n):
        go(remote(lat_ref, latv.at[own_block], tsend.at[k], trecv.at[k], me_y, to(k)))
        go(g_copy(k, 0))
        go(g_copy(k, 1))
    for k in range(1, n):
        go(remote(
            x_ref.at[:, rows(to(k) * feats, feats, 128)], cin.at[own_block],
            xsend.at[k], xrecv.at[k], me_y, to(k),
        ))

    def arrival(dst, ssem, rsem):
        return remote(dst, dst, ssem, rsem, other_y, x)

    def chunk_at(c):
        k, sub = divmod(c, subs)
        return source(k), k, sub

    def z_copy(slot, c):
        j, _, sub = chunk_at(c)
        span = rows(j * half + sub * CHUNK, CHUNK, CHUNK)
        return remote(
            gb.at[slot, span], gb.at[slot + 2, span], zsend.at[slot, c], zrecv.at[slot + 2, c], below, x
        )

    def z_arrival(slot, c):
        j, _, sub = chunk_at(c)
        dst = gb.at[slot, rows(j * half + sub * CHUNK, CHUNK, CHUNK)]
        return remote(dst, dst, zsend.at[slot - 2, c], zrecv.at[slot, c], other_y, x)

    def holds(d):
        return (a + d < LEVELS) if d == 0 else jnp.logical_and(a > 0, a + d < LEVELS)

    def flow(c):
        j, k, sub = chunk_at(c)
        if sub == 0:
            if k == 0:
                local[0].wait()
            else:
                g_arrival(k, 0).wait_recv()
            g_arrival(k, 1).wait_recv()

        @pl.when(a > 1)
        def _():
            z_copy(0, c).start()
            z_copy(1, c).start()

        for d in range(1, REACH):
            @pl.when(holds(d))
            def _():
                for slot in (2 * d, 2 * d + 1):
                    z_arrival(slot, c).wait_recv()
                    if d < REACH - 1:
                        @pl.when(a > 1)
                        def _():
                            z_copy(slot, c).start()

    def weight(ref, slot):
        return ref[slot : slot + 1, 0:1]

    def s0_copy(bb, c):
        j, _, sub = chunk_at(c)
        span = rows(j * half + sub * CHUNK, CHUNK, CHUNK)
        return remote(
            s0out.at[bb, span], s0in.at[bb, span], s0send.at[bb, c], s0recv.at[bb, c], below, x
        )

    def low_copy(bb, k):
        j = source(k)
        span = rows(j * half, half, half)
        src = lpeer.at[span] if bb else lown.at[rows(j * own_rows + h * half, half, half)]
        return remote(src, llow.at[bb, span], llsend.at[bb, k], llrecv.at[bb, k], above, x)

    def wlow_copy(bb):
        return remote(wpeer if bb else wrel_ref, wlow.at[bb], wlsend.at[bb], wlrecv.at[bb], above, x)

    def mlow_copy():
        return remote(mlow, mlowin, mlsend.at[0], mlrecv.at[0], below, x)

    def low_inner(c):
        j, k, sub = chunk_at(c)
        span = rows(j * half + sub * CHUNK, CHUNK, CHUNK)
        if sub == 0:
            for bb in range(2):
                low_copy(bb, k).wait_recv()

        @pl.loop(0, tiles)
        def _(t):
            cols = rows(t * TILE, TILE, 128)
            mine = llow[0, span, cols].astype(F32)
            theirs = llow[1, span, cols].astype(F32)
            for slot in range(SLOTS):
                values = gb[slot, span, cols].astype(F32)
                lowacc[slot + 2] += fold(values * mine)
                lowacc[8 + slot + 2] += fold(values * theirs)

    def combine(c):
        j, _, sub = chunk_at(c)
        span = rows(j * half + sub * CHUNK, CHUNK, CHUNK)
        @pl.when(a == 1)
        def _():
            @pl.loop(0, tiles)
            def _(t):
                cols = rows(t * TILE, TILE, 128)
                for bb in range(2):
                    value = jnp.zeros((CHUNK, TILE), F32)
                    for slot in range(SLOTS):
                        value = value + wlow[bb, slot + 2 : slot + 3, 0:1] * gb[slot, span, cols].astype(F32)
                    s0out[bb, span, cols] = value.astype(BF16)

            for bb in range(2):
                s0_copy(bb, c).start()

        for d in range(REACH):
            @pl.when(holds(d))
            def _():
                @pl.loop(0, tiles)
                def _(t):
                    cols = rows(t * TILE, TILE, 128)
                    first = gb[2 * d, span, cols].astype(F32)
                    second = gb[2 * d + 1, span, cols].astype(F32)
                    for bb, ref in ((0, wrel_ref), (1, wpeer)):
                        value = weight(ref, 2 * d) * first + weight(ref, 2 * d + 1) * second
                        if d:
                            value = sacc[bb, :, cols] + value
                        sacc[bb, :, cols] = value

        @pl.when(a == 0)
        def _():
            for bb in range(2):
                s0_copy(bb, c).wait_recv()

            @pl.loop(0, tiles)
            def _(t):
                cols = rows(t * TILE, TILE, 128)
                for bb in range(2):
                    sacc[bb, :, cols] += s0in[bb, span, cols].astype(F32)

        @pl.loop(0, tiles)
        def _(t):
            cols = rows(t * TILE, TILE, 128)
            og[rows(j * own_rows + h * half + sub * CHUNK, CHUNK, CHUNK), cols] = sacc[0, :, cols].astype(BF16)
            sout[span, cols] = sacc[1, :, cols].astype(BF16)

        go(remote(
            sout.at[span], og.at[rows(j * own_rows + h * half + sub * CHUNK, CHUNK, CHUNK)],
            ssend.at[c], srecv.at[c], other_y, x,
        ))

    def s_arrival(c):
        j, _, sub = chunk_at(c)
        return arrival(
            og.at[rows(j * own_rows + (1 - h) * half + sub * CHUNK, CHUNK, CHUNK)], ssend.at[c], srecv.at[c]
        )

    def inner(c):
        j, k, sub = chunk_at(c)
        span = rows(j * half + sub * CHUNK, CHUNK, CHUNK)
        own_span = rows(j * own_rows + h * half + sub * CHUNK, CHUNK, CHUNK)
        if sub == 0:
            arrival(lpeer.at[rows(j * half, half, half)], lsend.at[k], lrecv.at[k]).wait_recv()

            @pl.when(a == 0)
            def _():
                low_copy(1, k).start()
        for d in range(REACH):
            @pl.when(holds(d))
            def _():
                @pl.loop(0, tiles)
                def _(t):
                    cols = rows(t * TILE, TILE, 128)
                    mine = lown[own_span, cols].astype(F32)
                    theirs = lpeer[span, cols].astype(F32)
                    for slot in (2 * d, 2 * d + 1):
                        values = gb[slot, span, cols].astype(F32)
                        mixacc[slot] += fold(values * mine)
                        mixacc[8 + slot] += fold(values * theirs)

    mixacc[...] = jnp.zeros_like(mixacc)
    lowacc[...] = jnp.zeros_like(lowacc)
    local[2].wait()

    def square(t, total):
        part = xo[:, rows(t * TILE, TILE, 128)].astype(F32)
        part = part * part
        for at_col in range(0, TILE, 128):
            total = total + part[:, at_col : at_col + 128]
        return total

    lanes = lax.fori_loop(0, width // TILE, square, jnp.zeros((own_rows, 128), F32))
    mean_sq = jnp.sum(lanes, axis=1, keepdims=True) / width
    inv[own_block] = jnp.broadcast_to(lax.rsqrt(mean_sq + epsilon), (own_rows, 128))
    for k in range(1, n):
        go(remote(inv.at[own_block], inv.at[own_block], isend.at[k], irecv.at[k], me_y, to(k)))

    arrival(wpeer, wsem.at[0], wsem.at[1]).wait_recv()

    @pl.when(a == 0)
    def _():
        for bb in range(2):
            wlow_copy(bb).start()

    flow(0)

    local[1].wait()
    for k in range(1, n):
        arrival(latv.at[rows(source(k) * own_rows, own_rows, own_rows)], tsend.at[k], trecv.at[k]).wait_recv()
    _, own_slopes = gelu_pair(latv[own_block].astype(F32))
    slopes[...] = own_slopes
    for j in range(n):
        block = slice(j * own_rows, (j + 1) * own_rows)
        values, _ = gelu_pair(latv[block].astype(F32))
        actv[block] = values.astype(BF16)
    local[4].wait()
    local[3].wait()

    def layer_out(k):
        j = source(k)
        block = rows(j * own_rows, own_rows, own_rows)
        if k:
            arrival(cin.at[block], xsend.at[k], xrecv.at[k]).wait_recv()

        @pl.loop(0, tiles)
        def _(t):
            cols = rows(t * TILE, TILE, 128)
            branch = jnp.dot(actv[block, :], upv[:, cols], preferred_element_type=F32)
            lown[block, cols] = (cin[block, cols].astype(F32) + branch).astype(BF16)

        go(remote(
            lown.at[rows(j * own_rows + (1 - h) * half, half, half)], lpeer.at[rows(j * half, half, half)],
            lsend.at[k], lrecv.at[k], other_y, x,
        ))

        @pl.when(a == 0)
        def _():
            low_copy(0, k).start()

    def act_block(k):
        j = source(k)
        for sub in range(subs):
            s_arrival(k * subs + sub).wait_recv()
        part = lax.dot_general(
            og[rows(j * own_rows, own_rows, own_rows), :], upv[...], (((1,), (1,)), ((), ())),
            preferred_element_type=F32,
        )
        if k == 0:
            apown[...] = part
        else:
            apart[k] = part.astype(BF16)
            go(remote(apart.at[k], rsb.at[k], rsend.at[k], rrecv.at[k], me_y, j))

    layer_out(0)

    @pl.when(a == 1)
    def _():
        for bb in range(2):
            wlow_copy(bb).wait_recv()

    combine(0)
    for c in range(1, chunks):
        k, sub = divmod(c, subs)
        flow(c)
        combine(c)
        inner(c - 1)
        if sub == 0:
            layer_out(k)
            act_block(k - 1)
    inner(chunks - 1)
    act_block(n - 1)

    @pl.loop(0, tiles)
    def _(t):
        cols = rows(t * TILE, TILE, 128)
        upg_ref[:, cols] = lax.dot_general(
            actv[...], og[:, cols], (((0,), (0,)), ((), ())), preferred_element_type=F32
        ).astype(BF16)


    total = apown[...]
    for k in range(1, n):
        arrival(rsb.at[k], rsend.at[k], rrecv.at[k]).wait_recv()
        total = total + rsb[k].astype(F32)
    lg[own_block] = (total * slopes[...]).astype(BF16)
    for k in range(1, n):
        go(remote(lg.at[own_block], lg.at[own_block], asend.at[k], arecv.at[k], me_y, to(k)))

    @pl.when(a == 1)
    def _():
        for c in range(chunks):
            low_inner(c)
        for bb in range(2):
            for slot in range(8):
                mlow[bb, slot : slot + 1] = jnp.sum(lowacc[8 * bb + slot], axis=0, keepdims=True)
        mlow_copy().start()

    for bb in range(2):
        for slot in range(8):
            mst[bb, slot : slot + 1] = jnp.sum(mixacc[8 * bb + slot], axis=0, keepdims=True)

    mixlow[...] = jnp.zeros_like(mixlow)

    @pl.when(a == 0)
    def _():
        mlow_copy().wait_recv()
        mixlow[...] = mlowin[...]

    mst[...] = mst[...] + mixlow[...]
    go(remote(mst.at[1], mrecv_y, mysem.at[0], mysem.at[1], other_y, x))
    arrival(mrecv_y, mysem.at[0], mysem.at[1]).wait_recv()
    msx[...] = mst[0] + mrecv_y[...]
    for k in range(1, n):
        go(remote(msx, mrecv_dp.at[k], msend.at[k], mrecv.at[k], me_y, to(k)))

    mixed = msx[...]
    for k in range(1, n):
        arrival(mrecv_dp.at[k], msend.at[k], mrecv.at[k]).wait_recv()
        mixed = mixed + mrecv_dp[k]
    mix_ref[...] = mixed

    for k in range(1, n):
        block = rows(source(k) * own_rows, own_rows, own_rows)
        arrival(inv.at[block], isend.at[k], irecv.at[k]).wait_recv()
        arrival(lg.at[block], asend.at[k], arecv.at[k]).wait_recv()
    local[5].wait()

    @pl.loop(0, tiles)
    def _(t):
        cols = rows(t * TILE, TILE, 128)
        scaled = cin[:, cols].astype(F32) * inv[:, 0:1]
        normed = (scaled * gain_ref[:, cols].astype(F32)).astype(BF16)
        dng_ref[rows(t * TILE, TILE, 128), :] = lax.dot_general(
            normed, lg[...], (((0,), (0,)), ((), ())), preferred_element_type=F32
        ).astype(BF16)
        norm_grad = lax.dot_general(
            lg[...], downv[rows(t * TILE, TILE, 128), :], (((1,), (1,)), ((), ())),
            preferred_element_type=F32,
        )
        gaing_ref[:, cols] = jnp.sum(norm_grad * scaled, axis=0, keepdims=True)

    for copy in sends:
        copy.wait_send()

    @pl.when(a > 1)
    def _():
        for c in range(chunks):
            z_copy(0, c).wait_send()
            z_copy(1, c).wait_send()

    for d in range(1, REACH - 1):
        @pl.when(jnp.logical_and(a > 1, a + d < LEVELS))
        def _():
            for c in range(chunks):
                z_copy(2 * d, c).wait_send()
                z_copy(2 * d + 1, c).wait_send()

    @pl.when(a == 1)
    def _():
        mlow_copy().wait_send()
        for c in range(chunks):
            for bb in range(2):
                s0_copy(bb, c).wait_send()

    @pl.when(a == 0)
    def _():
        for bb in range(2):
            wlow_copy(bb).wait_send()
            for k in range(n):
                low_copy(bb, k).wait_send()


def local(layer_in, latent, mix_grad, down_proj, up_proj, norm_gain, mix_weight):
    _, own_rows, width = layer_in.shape
    n = lax.axis_size("dp")
    stride = lax.axis_size("section") // MIXES
    latents = latent.shape[2]
    feats = width // n
    tokens = own_rows * n
    chunks = tokens // 2 // CHUNK
    side = (lax.axis_index("section") // stride) % 2
    row = mix_weight[0]
    zero = jnp.zeros((1,), F32)
    rel = jnp.where(side == 1, jnp.concatenate([zero, row[:-1]]), row)
    rel = jnp.broadcast_to(rel[:, None], (MIXES, 128))
    dma = pltpu.SemaphoreType.DMA
    anyspace = pl.BlockSpec(memory_space=pl.ANY)
    vmem = pl.BlockSpec(memory_space=pltpu.VMEM)
    up_grad, down_grad, gain_grad, mixed = pl.pallas_call(
        functools.partial(kernel, n, stride),
        out_shape=(
            jax.ShapeDtypeStruct((latents, feats), BF16),
            jax.ShapeDtypeStruct((feats, latents), BF16),
            jax.ShapeDtypeStruct((1, feats), F32),
            jax.ShapeDtypeStruct((MIXES, 128), F32),
        ),
        in_specs=[anyspace] * 5 + [vmem] * 2,
        out_specs=(vmem,) * 4,
        scratch_shapes=[
            pltpu.VMEM((own_rows, width), BF16),
            pltpu.VMEM((tokens, feats), BF16),
            pltpu.VMEM((tokens, latents), BF16),
            pltpu.VMEM((SLOTS, tokens // 2, feats), BF16),
            pltpu.VMEM((tokens, 128), F32),
            pltpu.VMEM((tokens, latents), BF16),
            pltpu.VMEM((own_rows, latents), F32),
            pltpu.VMEM((tokens, feats), BF16),
            pltpu.VMEM((tokens // 2, feats), BF16),
            pltpu.VMEM((2, CHUNK, feats), F32),
            pltpu.VMEM((tokens // 2, feats), BF16),
            pltpu.VMEM((tokens, feats), BF16),
            pltpu.VMEM((16, 8, 128), F32),
            pltpu.VMEM((2, 8, 128), F32),
            pltpu.VMEM((8, 128), F32),
            pltpu.VMEM((8, 128), F32),
            pltpu.VMEM((n, 8, 128), F32),
            pltpu.VMEM((8, 128), F32),
            pltpu.VMEM((latents, feats), BF16),
            pltpu.VMEM((feats, latents), BF16),
            pltpu.VMEM((n, own_rows, latents), BF16),
            pltpu.VMEM((own_rows, latents), F32),
            pltpu.VMEM((n, own_rows, latents), BF16),
            pltpu.VMEM((tokens, latents), BF16),
            pltpu.VMEM((2, 8, 128), F32),
            pltpu.VMEM((2, tokens // 2, feats), BF16),
            pltpu.VMEM((16, 8, 128), F32),
            pltpu.VMEM((2, tokens // 2, feats), BF16),
            pltpu.VMEM((2, tokens // 2, feats), BF16),
            pltpu.VMEM((2, 8, 128), F32),
            pltpu.VMEM((2, 8, 128), F32),
            pltpu.VMEM((2, 8, 128), F32),
            dma((6,)),
            dma((2 * n,)), dma((2 * n,)),
            dma((n,)), dma((n,)),
            dma((n,)), dma((n,)),
            dma((n,)), dma((n,)),
            dma((2,)),
            dma((SLOTS, chunks)), dma((SLOTS, chunks)),
            dma((2,)), dma((2,)),
            dma((2, n)), dma((2, n)),
            dma((2, chunks)), dma((2, chunks)),
            dma((1,)), dma((1,)),
            dma((chunks,)), dma((chunks,)),
            dma((n,)), dma((n,)),
            dma((n,)), dma((n,)),
            dma((n,)), dma((n,)),
            dma((2,)),
            dma((n,)), dma((n,)),
        ],
        compiler_params=pltpu.CompilerParams(
            collective_id=0, has_side_effects=True, vmem_limit_bytes=60 * 1024 * 1024
        ),
    )(layer_in[0], latent[0], mix_grad[0], down_proj[0], up_proj[0], norm_gain, rel)
    sums = jnp.sum(mixed, axis=1)
    mixing = jnp.where(side == 1, jnp.concatenate([sums[1:], zero]), sums)
    return (up_grad[None], down_grad[None], gain_grad, mixing[None])


def solution(mesh):
    return jax.shard_map(
        local,
        mesh=mesh,
        in_specs=(
            P("section", "dp", None),
            P("section", "dp", None),
            P("section", "dp", None),
            P("section", "dp", None),
            P("section", None, "dp"),
            P("section", "dp"),
            P("section", None),
        ),
        out_specs=(
            P("section", None, "dp"),
            P("section", "dp", None),
            P("section", "dp"),
            P("section", None),
        ),
        check_vma=False,
    )
```

```python
import functools

import jax
import jax.numpy as jnp
from jax import lax
from jax.experimental import pallas as pl
from jax.experimental.pallas import tpu as pltpu
from jax.sharding import PartitionSpec as P

MIXES = 8
LEVELS = MIXES // 2
REACH = LEVELS - 1
SLOTS = 2 * REACH
CHUNK = 16
TILE = 640

epsilon = 1e-06
root_coef = 0.7978845608028654
MESH = pl.DeviceIdType.MESH
F32 = jnp.float32
BF16 = jnp.bfloat16


def gelu_pair(values):
    tangent = jnp.tanh(root_coef * (values + 0.044715 * values * values * values))
    result = 0.5 * values * (1.0 + tangent)
    slopes = 0.5 * (1.0 + tangent) + 0.5 * values * (1.0 - tangent * tangent) * root_coef * (
        1.0 + 3.0 * 0.044715 * values * values
    )
    return (result, slopes)


def fold(values):
    rows, cols = values.shape
    total = jnp.sum(values.reshape(rows // 8, 8, cols), axis=0)
    out = total[:, 0:128]
    for at in range(128, cols, 128):
        out = out + total[:, at : at + 128]
    return out


def kernel(
    n, stride,
    x_ref, lat_ref, g_ref, down_ref, up_ref, gain_ref, mw_ref,
    upg_ref, dng_ref, gaing_ref, mix_ref,
    xo, cin, latv, gb, inv, actv, slopes, lown, lpeer, sacc, sout, og, mixacc,
    mst, mrecv_y, msx, mrecv_dp, wpeer, upv, downv, apart, apown, rsb, lg,
    wown, wlow, llow, lowacc, s0out, s0in, mixlow, mlow, mlowin,
    loc, gsend, grecv, xsend, xrecv, tsend, trecv, isend, irecv, wsem, zsend, zrecv,
    wlsend, wlrecv, llsend, llrecv, s0send, s0recv, mlsend, mlrecv,
    ssend, srecv, lsend, lrecv, rsend, rrecv, asend, arecv, mysem, msend, mrecv,
):
    own_rows, width = x_ref.shape
    feats = width // n
    half = own_rows // 2
    subs = half // CHUNK
    chunks = n * subs
    tiles = feats // TILE

    sec = lax.axis_index("section")
    x = lax.axis_index("dp")
    q = sec // stride
    res = sec % stride
    a = q // 2
    h = q % 2

    def at(level, side):
        return (2 * level + side) * stride + res

    me_y = sec
    other_y = at(a, 1 - h)
    above = at(a + 1, h)
    below = at(a - 1, h)

    def dev(section, dp):
        return {"section": section, "dp": dp}

    def to(k):
        return lax.rem(x + k, n)

    def source(k):
        return lax.rem(x + n - k, n)

    def remote(src, dst, ssem, rsem, section, dp):
        return pltpu.make_async_remote_copy(
            src_ref=src, dst_ref=dst, send_sem=ssem, recv_sem=rsem,
            device_id=dev(section, dp), device_id_type=MESH,
        )

    def rows(start, size, unit):
        return pl.ds(pl.multiple_of(start, unit), size)

    barrier = pltpu.get_barrier_semaphore()
    for k in range(n):
        for e in range(2):
            if k or e:
                pl.semaphore_signal(
                    barrier, inc=1, device_id=dev(other_y if e else me_y, to(k)), device_id_type=MESH
                )

    @pl.when(a > 0)
    def _():
        pl.semaphore_signal(barrier, inc=1, device_id=dev(below, x), device_id_type=MESH)

    @pl.when(a < LEVELS - 1)
    def _():
        pl.semaphore_signal(barrier, inc=1, device_id=dev(above, x), device_id_type=MESH)

    @pl.when(h == 0)
    def _():
        for slot in range(MIXES):
            wown[slot : slot + 1] = jnp.broadcast_to(mw_ref[0:1, slot : slot + 1], (1, 128))

    @pl.when(h == 1)
    def _():
        wown[0:1] = jnp.zeros((1, 128), F32)
        for slot in range(1, MIXES):
            wown[slot : slot + 1] = jnp.broadcast_to(mw_ref[0:1, slot - 1 : slot], (1, 128))

    own_cols = rows(x * feats, feats, 128)
    own_block = rows(x * own_rows, own_rows, own_rows)
    local = [
        pltpu.make_async_copy(
            g_ref.at[rows(h * half, half, half), own_cols], gb.at[h, rows(x * half, half, half)], loc.at[0]
        ),
        pltpu.make_async_copy(lat_ref, latv.at[own_block], loc.at[1]),
        pltpu.make_async_copy(x_ref, xo, loc.at[2]),
        pltpu.make_async_copy(x_ref.at[:, own_cols], cin.at[own_block], loc.at[3]),
        pltpu.make_async_copy(up_ref, upv, loc.at[4]),
        pltpu.make_async_copy(down_ref, downv, loc.at[5]),
    ]
    for copy in local:
        copy.start()

    neighbours = jnp.where(a > 0, 1, 0) + jnp.where(a < LEVELS - 1, 1, 0)
    pl.semaphore_wait(barrier, 2 * n - 1 + neighbours)

    sends = []

    def go(copy):
        copy.start()
        sends.append(copy)
        return copy

    def g_copy(k, e):
        side = 1 - h if e else h
        return remote(
            g_ref.at[rows(side * half, half, half), rows(to(k) * feats, feats, 128)],
            gb.at[h, rows(x * half, half, half)],
            gsend.at[e * n + k], grecv.at[e * n + k],
            other_y if e else me_y, to(k),
        )

    def g_arrival(k, e):
        slot = 1 - h if e else h
        dst = gb.at[slot, rows(source(k) * half, half, half)]
        return remote(dst, dst, gsend.at[e * n + k], grecv.at[e * n + k], me_y, to(k) if k else x)

    go(g_copy(0, 1))
    w_copy = go(remote(wown, wpeer, wsem.at[0], wsem.at[1], other_y, x))
    for k in range(1, n):
        go(remote(lat_ref, latv.at[own_block], tsend.at[k], trecv.at[k], me_y, to(k)))
        go(g_copy(k, 0))
        go(g_copy(k, 1))
    for k in range(1, n):
        go(remote(
            x_ref.at[:, rows(to(k) * feats, feats, 128)], cin.at[own_block],
            xsend.at[k], xrecv.at[k], me_y, to(k),
        ))

    def arrival(dst, ssem, rsem):
        return remote(dst, dst, ssem, rsem, other_y, x)

    def chunk_at(c):
        k, sub = divmod(c, subs)
        return source(k), k, sub

    def z_copy(slot, c):
        j, _, sub = chunk_at(c)
        span = rows(j * half + sub * CHUNK, CHUNK, CHUNK)
        return remote(
            gb.at[slot, span], gb.at[slot + 2, span], zsend.at[slot, c], zrecv.at[slot + 2, c], below, x
        )

    def z_arrival(slot, c):
        j, _, sub = chunk_at(c)
        dst = gb.at[slot, rows(j * half + sub * CHUNK, CHUNK, CHUNK)]
        return remote(dst, dst, zsend.at[slot - 2, c], zrecv.at[slot, c], other_y, x)

    def holds(d):
        return (a + d < LEVELS) if d == 0 else jnp.logical_and(a > 0, a + d < LEVELS)

    def flow(c):
        j, k, sub = chunk_at(c)
        if sub == 0:
            if k == 0:
                local[0].wait()
            else:
                g_arrival(k, 0).wait_recv()
            g_arrival(k, 1).wait_recv()

        @pl.when(a > 1)
        def _():
            z_copy(0, c).start()
            z_copy(1, c).start()

        for d in range(1, REACH):
            @pl.when(holds(d))
            def _():
                for slot in (2 * d, 2 * d + 1):
                    z_arrival(slot, c).wait_recv()
                    if d < REACH - 1:
                        @pl.when(a > 1)
                        def _():
                            z_copy(slot, c).start()

    def weight(ref, slot):
        return ref[slot : slot + 1, 0:1]

    def s0_copy(bb, c):
        j, _, sub = chunk_at(c)
        span = rows(j * half + sub * CHUNK, CHUNK, CHUNK)
        return remote(
            s0out.at[bb, span], s0in.at[bb, span], s0send.at[bb, c], s0recv.at[bb, c], below, x
        )

    def low_copy(bb, k):
        j = source(k)
        span = rows(j * half, half, half)
        src = lpeer.at[span] if bb else lown.at[rows(j * own_rows + h * half, half, half)]
        return remote(src, llow.at[bb, span], llsend.at[bb, k], llrecv.at[bb, k], above, x)

    def wlow_copy(bb):
        return remote(wpeer if bb else wown, wlow.at[bb], wlsend.at[bb], wlrecv.at[bb], above, x)

    def mlow_copy():
        return remote(mlow, mlowin, mlsend.at[0], mlrecv.at[0], below, x)

    def low_inner(c):
        j, k, sub = chunk_at(c)
        span = rows(j * half + sub * CHUNK, CHUNK, CHUNK)
        if sub == 0:
            for bb in range(2):
                low_copy(bb, k).wait_recv()

        @pl.loop(0, tiles)
        def _(t):
            cols = rows(t * TILE, TILE, 128)
            mine = llow[0, span, cols].astype(F32)
            theirs = llow[1, span, cols].astype(F32)
            for slot in range(SLOTS):
                values = gb[slot, span, cols].astype(F32)
                lowacc[slot + 2] += fold(values * mine)
                lowacc[8 + slot + 2] += fold(values * theirs)

    def combine(c):
        j, _, sub = chunk_at(c)
        span = rows(j * half + sub * CHUNK, CHUNK, CHUNK)
        @pl.when(a == 1)
        def _():
            @pl.loop(0, tiles)
            def _(t):
                cols = rows(t * TILE, TILE, 128)
                for bb in range(2):
                    value = jnp.zeros((CHUNK, TILE), F32)
                    for slot in range(SLOTS):
                        value = value + wlow[bb, slot + 2 : slot + 3, 0:1] * gb[slot, span, cols].astype(F32)
                    s0out[bb, span, cols] = value.astype(BF16)

            for bb in range(2):
                s0_copy(bb, c).start()

        for d in range(REACH):
            @pl.when(holds(d))
            def _():
                @pl.loop(0, tiles)
                def _(t):
                    cols = rows(t * TILE, TILE, 128)
                    first = gb[2 * d, span, cols].astype(F32)
                    second = gb[2 * d + 1, span, cols].astype(F32)
                    for bb, ref in ((0, wown), (1, wpeer)):
                        value = weight(ref, 2 * d) * first + weight(ref, 2 * d + 1) * second
                        if d:
                            value = sacc[bb, :, cols] + value
                        sacc[bb, :, cols] = value

        @pl.when(a == 0)
        def _():
            for bb in range(2):
                s0_copy(bb, c).wait_recv()

            @pl.loop(0, tiles)
            def _(t):
                cols = rows(t * TILE, TILE, 128)
                for bb in range(2):
                    sacc[bb, :, cols] += s0in[bb, span, cols].astype(F32)

        @pl.loop(0, tiles)
        def _(t):
            cols = rows(t * TILE, TILE, 128)
            og[rows(j * own_rows + h * half + sub * CHUNK, CHUNK, CHUNK), cols] = sacc[0, :, cols].astype(BF16)
            sout[span, cols] = sacc[1, :, cols].astype(BF16)

        go(remote(
            sout.at[span], og.at[rows(j * own_rows + h * half + sub * CHUNK, CHUNK, CHUNK)],
            ssend.at[c], srecv.at[c], other_y, x,
        ))

    def s_arrival(c):
        j, _, sub = chunk_at(c)
        return arrival(
            og.at[rows(j * own_rows + (1 - h) * half + sub * CHUNK, CHUNK, CHUNK)], ssend.at[c], srecv.at[c]
        )

    def inner(c):
        j, k, sub = chunk_at(c)
        span = rows(j * half + sub * CHUNK, CHUNK, CHUNK)
        own_span = rows(j * own_rows + h * half + sub * CHUNK, CHUNK, CHUNK)
        if sub == 0:
            arrival(lpeer.at[rows(j * half, half, half)], lsend.at[k], lrecv.at[k]).wait_recv()

            @pl.when(a == 0)
            def _():
                low_copy(1, k).start()
        for d in range(REACH):
            @pl.when(holds(d))
            def _():
                @pl.loop(0, tiles)
                def _(t):
                    cols = rows(t * TILE, TILE, 128)
                    mine = lown[own_span, cols].astype(F32)
                    theirs = lpeer[span, cols].astype(F32)
                    for slot in (2 * d, 2 * d + 1):
                        values = gb[slot, span, cols].astype(F32)
                        mixacc[slot] += fold(values * mine)
                        mixacc[8 + slot] += fold(values * theirs)

    mixacc[...] = jnp.zeros_like(mixacc)
    lowacc[...] = jnp.zeros_like(lowacc)
    local[2].wait()

    def square(t, total):
        part = xo[:, rows(t * TILE, TILE, 128)].astype(F32)
        part = part * part
        for at_col in range(0, TILE, 128):
            total = total + part[:, at_col : at_col + 128]
        return total

    lanes = lax.fori_loop(0, width // TILE, square, jnp.zeros((own_rows, 128), F32))
    mean_sq = jnp.sum(lanes, axis=1, keepdims=True) / width
    inv[own_block] = jnp.broadcast_to(lax.rsqrt(mean_sq + epsilon), (own_rows, 128))
    for k in range(1, n):
        go(remote(inv.at[own_block], inv.at[own_block], isend.at[k], irecv.at[k], me_y, to(k)))

    arrival(wpeer, wsem.at[0], wsem.at[1]).wait_recv()

    @pl.when(a == 0)
    def _():
        for bb in range(2):
            wlow_copy(bb).start()

    flow(0)

    local[1].wait()
    for k in range(1, n):
        arrival(latv.at[rows(source(k) * own_rows, own_rows, own_rows)], tsend.at[k], trecv.at[k]).wait_recv()
    _, own_slopes = gelu_pair(latv[own_block].astype(F32))
    slopes[...] = own_slopes
    for j in range(n):
        block = slice(j * own_rows, (j + 1) * own_rows)
        values, _ = gelu_pair(latv[block].astype(F32))
        actv[block] = values.astype(BF16)
    local[4].wait()
    local[3].wait()

    def layer_out(k):
        j = source(k)
        block = rows(j * own_rows, own_rows, own_rows)
        if k:
            arrival(cin.at[block], xsend.at[k], xrecv.at[k]).wait_recv()

        @pl.loop(0, tiles)
        def _(t):
            cols = rows(t * TILE, TILE, 128)
            branch = jnp.dot(actv[block, :], upv[:, cols], preferred_element_type=F32)
            lown[block, cols] = (cin[block, cols].astype(F32) + branch).astype(BF16)

        go(remote(
            lown.at[rows(j * own_rows + (1 - h) * half, half, half)], lpeer.at[rows(j * half, half, half)],
            lsend.at[k], lrecv.at[k], other_y, x,
        ))

        @pl.when(a == 0)
        def _():
            low_copy(0, k).start()

    def act_block(k):
        j = source(k)
        for sub in range(subs):
            s_arrival(k * subs + sub).wait_recv()
        part = lax.dot_general(
            og[rows(j * own_rows, own_rows, own_rows), :], upv[...], (((1,), (1,)), ((), ())),
            preferred_element_type=F32,
        )
        if k == 0:
            apown[...] = part
        else:
            apart[k] = part.astype(BF16)
            go(remote(apart.at[k], rsb.at[k], rsend.at[k], rrecv.at[k], me_y, j))

    layer_out(0)

    @pl.when(a == 1)
    def _():
        for bb in range(2):
            wlow_copy(bb).wait_recv()

    combine(0)
    for c in range(1, chunks):
        k, sub = divmod(c, subs)
        flow(c)
        combine(c)
        inner(c - 1)
        if sub == 0:
            layer_out(k)
            act_block(k - 1)
        if c >= subs:
            @pl.when(a == 1)
            def _():
                low_inner(c - subs)
    inner(chunks - 1)
    act_block(n - 1)

    @pl.when(a == 1)
    def _():
        for c in range(chunks - subs, chunks):
            low_inner(c)
        for bb in range(2):
            for slot in range(8):
                mlow[bb, slot : slot + 1] = jnp.sum(lowacc[8 * bb + slot], axis=0, keepdims=True)
        mlow_copy().start()

    for bb in range(2):
        for slot in range(8):
            mst[bb, slot : slot + 1] = jnp.sum(mixacc[8 * bb + slot], axis=0, keepdims=True)

    @pl.loop(0, tiles)
    def _(t):
        cols = rows(t * TILE, TILE, 128)
        upg_ref[:, cols] = lax.dot_general(
            actv[...], og[:, cols], (((0,), (0,)), ((), ())), preferred_element_type=F32
        ).astype(BF16)


    total = apown[...]
    for k in range(1, n):
        arrival(rsb.at[k], rsend.at[k], rrecv.at[k]).wait_recv()
        total = total + rsb[k].astype(F32)
    lg[own_block] = (total * slopes[...]).astype(BF16)
    for k in range(1, n):
        go(remote(lg.at[own_block], lg.at[own_block], asend.at[k], arecv.at[k], me_y, to(k)))

    mixlow[...] = jnp.zeros_like(mixlow)

    @pl.when(a == 0)
    def _():
        mlow_copy().wait_recv()
        mixlow[...] = mlowin[...]

    mst[...] = mst[...] + mixlow[...]
    go(remote(mst.at[1], mrecv_y, mysem.at[0], mysem.at[1], other_y, x))
    for k in range(1, n):
        block = rows(source(k) * own_rows, own_rows, own_rows)
        arrival(inv.at[block], isend.at[k], irecv.at[k]).wait_recv()
        arrival(lg.at[block], asend.at[k], arecv.at[k]).wait_recv()
    local[5].wait()

    arrival(mrecv_y, mysem.at[0], mysem.at[1]).wait_recv()
    msx[...] = mst[0] + mrecv_y[...]
    for k in range(1, n):
        go(remote(msx, mrecv_dp.at[k], msend.at[k], mrecv.at[k], me_y, to(k)))

    @pl.loop(0, tiles)
    def _(t):
        cols = rows(t * TILE, TILE, 128)
        scaled = cin[:, cols].astype(F32) * inv[:, 0:1]
        normed = (scaled * gain_ref[:, cols].astype(F32)).astype(BF16)
        dng_ref[rows(t * TILE, TILE, 128), :] = lax.dot_general(
            normed, lg[...], (((0,), (0,)), ((), ())), preferred_element_type=F32
        ).astype(BF16)
        norm_grad = lax.dot_general(
            lg[...], downv[rows(t * TILE, TILE, 128), :], (((1,), (1,)), ((), ())),
            preferred_element_type=F32,
        )
        gaing_ref[:, cols] = jnp.sum(norm_grad * scaled, axis=0, keepdims=True)

    mixed = msx[...]
    for k in range(1, n):
        arrival(mrecv_dp.at[k], msend.at[k], mrecv.at[k]).wait_recv()
        mixed = mixed + mrecv_dp[k]
    sums = jnp.sum(mixed, axis=1, keepdims=True)
    lane = lax.broadcasted_iota(jnp.int32, (1, MIXES), 1)

    def mix_row(shift):
        row = jnp.zeros((1, MIXES), F32)
        for m in range(MIXES - shift):
            row = jnp.where(lane == m, sums[m + shift : m + shift + 1, 0:1], row)
        mix_ref[...] = row

    @pl.when(h == 0)
    def _():
        mix_row(0)

    @pl.when(h == 1)
    def _():
        mix_row(1)

    for copy in sends:
        copy.wait_send()

    @pl.when(a > 1)
    def _():
        for c in range(chunks):
            z_copy(0, c).wait_send()
            z_copy(1, c).wait_send()

    for d in range(1, REACH - 1):
        @pl.when(jnp.logical_and(a > 1, a + d < LEVELS))
        def _():
            for c in range(chunks):
                z_copy(2 * d, c).wait_send()
                z_copy(2 * d + 1, c).wait_send()

    @pl.when(a == 1)
    def _():
        mlow_copy().wait_send()
        for c in range(chunks):
            for bb in range(2):
                s0_copy(bb, c).wait_send()

    @pl.when(a == 0)
    def _():
        for bb in range(2):
            wlow_copy(bb).wait_send()
            for k in range(n):
                low_copy(bb, k).wait_send()


def local(layer_in, latent, mix_grad, down_proj, up_proj, norm_gain, mix_weight):
    _, own_rows, width = layer_in.shape
    n = lax.axis_size("dp")
    stride = lax.axis_size("section") // MIXES
    latents = latent.shape[2]
    feats = width // n
    tokens = own_rows * n
    chunks = tokens // 2 // CHUNK
    dma = pltpu.SemaphoreType.DMA
    anyspace = pl.BlockSpec(memory_space=pl.ANY)
    vmem = pl.BlockSpec(memory_space=pltpu.VMEM)
    up_grad, down_grad, gain_grad, mixed = pl.pallas_call(
        functools.partial(kernel, n, stride),
        out_shape=(
            jax.ShapeDtypeStruct((latents, feats), BF16),
            jax.ShapeDtypeStruct((feats, latents), BF16),
            jax.ShapeDtypeStruct((1, feats), F32),
            jax.ShapeDtypeStruct((1, MIXES), F32),
        ),
        in_specs=[anyspace] * 5 + [vmem] * 2,
        out_specs=(vmem,) * 4,
        scratch_shapes=[
            pltpu.VMEM((own_rows, width), BF16),
            pltpu.VMEM((tokens, feats), BF16),
            pltpu.VMEM((tokens, latents), BF16),
            pltpu.VMEM((SLOTS, tokens // 2, feats), BF16),
            pltpu.VMEM((tokens, 128), F32),
            pltpu.VMEM((tokens, latents), BF16),
            pltpu.VMEM((own_rows, latents), F32),
            pltpu.VMEM((tokens, feats), BF16),
            pltpu.VMEM((tokens // 2, feats), BF16),
            pltpu.VMEM((2, CHUNK, feats), F32),
            pltpu.VMEM((tokens // 2, feats), BF16),
            pltpu.VMEM((tokens, feats), BF16),
            pltpu.VMEM((16, 8, 128), F32),
            pltpu.VMEM((2, 8, 128), F32),
            pltpu.VMEM((8, 128), F32),
            pltpu.VMEM((8, 128), F32),
            pltpu.VMEM((n, 8, 128), F32),
            pltpu.VMEM((8, 128), F32),
            pltpu.VMEM((latents, feats), BF16),
            pltpu.VMEM((feats, latents), BF16),
            pltpu.VMEM((n, own_rows, latents), BF16),
            pltpu.VMEM((own_rows, latents), F32),
            pltpu.VMEM((n, own_rows, latents), BF16),
            pltpu.VMEM((tokens, latents), BF16),
            pltpu.VMEM((8, 128), F32),
            pltpu.VMEM((2, 8, 128), F32),
            pltpu.VMEM((2, tokens // 2, feats), BF16),
            pltpu.VMEM((16, 8, 128), F32),
            pltpu.VMEM((2, tokens // 2, feats), BF16),
            pltpu.VMEM((2, tokens // 2, feats), BF16),
            pltpu.VMEM((2, 8, 128), F32),
            pltpu.VMEM((2, 8, 128), F32),
            pltpu.VMEM((2, 8, 128), F32),
            dma((6,)),
            dma((2 * n,)), dma((2 * n,)),
            dma((n,)), dma((n,)),
            dma((n,)), dma((n,)),
            dma((n,)), dma((n,)),
            dma((2,)),
            dma((SLOTS, chunks)), dma((SLOTS, chunks)),
            dma((2,)), dma((2,)),
            dma((2, n)), dma((2, n)),
            dma((2, chunks)), dma((2, chunks)),
            dma((1,)), dma((1,)),
            dma((chunks,)), dma((chunks,)),
            dma((n,)), dma((n,)),
            dma((n,)), dma((n,)),
            dma((n,)), dma((n,)),
            dma((2,)),
            dma((n,)), dma((n,)),
        ],
        compiler_params=pltpu.CompilerParams(
            collective_id=0, has_side_effects=True, vmem_limit_bytes=60 * 1024 * 1024
        ),
    )(layer_in[0], latent[0], mix_grad[0], down_proj[0], up_proj[0], norm_gain, mix_weight)
    return (up_grad[None], down_grad[None], gain_grad, mixed)


def solution(mesh):
    return jax.shard_map(
        local,
        mesh=mesh,
        in_specs=(
            P("section", "dp", None),
            P("section", "dp", None),
            P("section", "dp", None),
            P("section", "dp", None),
            P("section", None, "dp"),
            P("section", "dp"),
            P("section", None),
        ),
        out_specs=(
            P("section", None, "dp"),
            P("section", "dp", None),
            P("section", "dp"),
            P("section", None),
        ),
        check_vma=False,
    )
```
